32 devices in a mesh: groups: 2 (over y), blk: 4 (over z), rep: 2 (over x), sub: 2 (over core).
Axes of the slice: x: 2, y: 2, z: 4, core: 2. Of those that a mesh axis runs over, the one named last changes fastest.
Arguments:
- replica_delta: bfloat16 [32, 32, 4608], P(('groups', 'blk', 'rep', 'sub')), parts along dimension 0, may hold values from -150 to 150
- momentum: float32 [64, 4608], P(('groups', 'blk')), parts along dimension 0, may hold values from -6 to 6
- params: float32 [64, 4608], P(('groups', 'blk')), parts along dimension 0, may hold values from -6 to 6
- prev_master: float32 [64, 4608], P(('groups', 'blk')), parts along dimension 0, may hold values from -6 to 6
Outputs:
- new_params: float32 [64, 4608], P(('groups', 'blk')), parts along dimension 0
- new_momentum: float32 [64, 4608], P(('groups', 'blk')), parts along dimension 0
- prev_weights: bfloat16 [64, 4608], P('groups'), parts along dimension 0
The draws below stay inside these ranges and needn't reach their ends.
There are 2 independent parts, one for each index of `groups`. The reference program is written for one: setup_inputs(seed, part) draws one part's arguments, and reference() takes and returns one part's arrays. A program takes and returns all parts, laid end to end along the dimension named above; each array names one. Nothing has to cross between parts.
All inputs are finite; a program needn't handle non-finite values.
Results may differ from the reference program's by a relative error of at most 0.012.
Values may be sent and summed in bfloat16 or wider, within the bound.
No kernel may reach another device: no remote copies, remote signals or barrier semaphores. Data moves between devices by JAX's collectives and lax.ppermute only.
A program may use at most 64 MiB of HBM per device.

```python
import math
import jax
import jax.numpy as jnp
from jax import lax

D = 4608
ROW_OWN = 8
LROWS = 32
REPLICAS = 16


def draw_replica_delta(key, part):
    base_key = jax.random.fold_in(key, 11)
    key_rows, key_cols, key_noise, key_shared, key_blocks = jax.random.split(base_key, 5)
    trend = jnp.power(3.0, jnp.arange(LROWS, dtype=jnp.float32) / max(LROWS - 1, 1))
    row_scale = jnp.exp(jax.random.uniform(key_rows, (LROWS,), jnp.float32) * math.log(10.0)) * trend
    col_scale = jnp.exp(jax.random.uniform(key_cols, (D,), jnp.float32) * math.log(10.0))
    block_count = LROWS // ROW_OWN
    chosen = jax.random.permutation(key_blocks, block_count) < block_count // 2
    indep = jax.random.normal(key_noise, (REPLICAS, LROWS, D), jnp.float32)
    shared = jax.random.normal(key_shared, (1, LROWS, D), jnp.float32)
    target = 9.0
    rho_square = min(target / max(REPLICAS - 1, 1), 0.9)
    block_rho = jnp.where(chosen, jnp.float32(math.sqrt(rho_square)), jnp.float32(0.0))
    row_rho = jnp.repeat(block_rho, ROW_OWN)[None, :, None]
    noise = row_rho * shared + jnp.sqrt(1.0 - row_rho * row_rho) * indep
    noise = jnp.clip(noise, -4.0, 4.0)
    values = noise * row_scale[None, :, None] * col_scale[None, None, :] / 8.0
    return values.astype(jnp.bfloat16)


def levels(own_key, dims, pieces, low, high):
    def one(dim, parts):
        draws = jax.random.uniform(jax.random.fold_in(jax.random.fold_in(own_key, 6), dim), (parts,), jnp.float32, low / len(pieces), high / len(pieces))
        return jnp.repeat(jnp.exp(draws), dims[dim] // parts).reshape((-1,) + (1,) * (len(dims) - dim - 1))

    factor_of = one(*pieces[0])
    for cut in pieces[1:]:
        factor_of = factor_of * one(*cut)
    return factor_of


def gaussian(stream_key, extent, deviation, limit, shards=(), held_as=jnp.bfloat16):
    result = deviation * jax.random.normal(stream_key, extent, jnp.float32)
    if shards:
        result = result * levels(stream_key, extent, shards, -0.22, 0.18)
    return jnp.clip(result, -limit, limit).astype(held_as)


def setup_inputs(seed: int = 0, part: int = 0) -> dict:
    keys = jax.random.split(jax.random.key(seed), 5)
    part_splits = jax.random.split(jax.random.fold_in(keys[4], part), 5)
    return {
        "replica_delta": draw_replica_delta(jax.random.fold_in(jax.random.fold_in(keys[4], part), 71), part),
        "momentum": gaussian(part_splits[1], (LROWS, D), 1.0, 6.0, ((0, 4),), jnp.float32),
        "params": gaussian(part_splits[2], (LROWS, D), 1.0, 6.0, ((0, 4),), jnp.float32),
        "prev_master": gaussian(part_splits[3], (LROWS, D), 1.0, 6.0, ((0, 4),), jnp.float32),
    }


momentum_coef = 0.9
outer_rate = 0.7

def reference(replica_delta, momentum, params, prev_master):
    summed = lax.optimization_barrier(jnp.sum(replica_delta, axis=0, dtype=jnp.float32))
    squares = jnp.sum(summed * summed)
    entries = replica_delta.shape[1] * replica_delta.shape[2]
    clip_factor = jnp.minimum(jnp.float32(1.0), jnp.sqrt(jnp.float32(entries)) / jnp.sqrt(squares + 1e-06))
    scaled = clip_factor * summed
    new_momentum = momentum_coef * momentum + scaled
    new_params = params - outer_rate * (scaled + momentum_coef * new_momentum)
    prev_weights = prev_master.astype(jnp.bfloat16)
    return (new_params, new_momentum, prev_weights)
```

```python
import jax
import jax.numpy as jnp
from jax import lax
from jax.sharding import PartitionSpec as P

momentum_coef = 0.9
outer_rate = 0.7
F32 = jnp.float32
BF16 = jnp.bfloat16
BLK_DIRECT = False


def swap(value, axis, size, bit):
    return lax.ppermute(value, axis, [(i, i ^ bit) for i in range(size)])


def bits_of(size):
    return [1 << k for k in range(size.bit_length() - 1)]


def make(mesh):
    n_blk, n_rep, n_sub = mesh.shape["blk"], mesh.shape["rep"], mesh.shape["sub"]

    def halves(value, axis, size, bit):
        index = lax.axis_index(axis)
        half = value.shape[1] // 2
        mine = (index // bit) % 2
        keep = lax.dynamic_slice_in_dim(value, mine * half, half, 1)
        away = lax.dynamic_slice_in_dim(value, (1 - mine) * half, half, 1)
        return keep, away

    def joined(own, other, axis, bit, dim):
        upper = (lax.axis_index(axis) // bit) % 2 == 1
        return jnp.concatenate(
            [jnp.where(upper, other, own), jnp.where(upper, own, other)], axis=dim
        )

    def per_device(replica_delta, momentum, params, prev_master):
        delta = replica_delta[0]
        rows = momentum.shape[0]
        entries = delta.shape[0] * delta.shape[1]
        blk = lax.axis_index("blk")

        other = swap(delta, "sub", n_sub, 1)
        total = delta.astype(F32) + other.astype(F32)
        total, _ = halves(total, "sub", n_sub, 1)
        for bit in reversed(bits_of(n_rep)):
            keep, away = halves(total, "rep", n_rep, bit)
            total = keep + swap(away.astype(BF16), "rep", n_rep, bit).astype(F32)
        if BLK_DIRECT:
            sent = total.astype(BF16)
            for k in range(1, n_blk):
                total = total + swap(sent, "blk", n_blk, k).astype(F32)
        else:
            for bit in bits_of(n_blk):
                total = total + swap(total.astype(BF16), "blk", n_blk, bit).astype(F32)
        squares = jnp.sum(total * total)
        own = lax.dynamic_slice_in_dim(total, blk * rows, rows, 0)

        for axis, size in (("rep", n_rep), ("sub", n_sub)):
            for bit in bits_of(size):
                packed = jnp.concatenate([own, jnp.full((rows, 128), squares, F32)], axis=1)
                got = swap(packed, axis, size, bit)
                width = own.shape[1]
                own = joined(own, got[:, :width], axis, bit, 1)
                squares = squares + got[0, width]

        clip_factor = jnp.minimum(
            jnp.float32(1.0), jnp.sqrt(jnp.float32(entries)) / jnp.sqrt(squares + 1e-06)
        )
        scaled = clip_factor * own
        new_momentum = momentum_coef * momentum + scaled
        new_params = params - outer_rate * (scaled + momentum_coef * new_momentum)

        prev = prev_master.astype(BF16)
        prev, _ = halves(prev, "sub", n_sub, 1)
        for bit in reversed(bits_of(n_rep)):
            prev, _ = halves(prev, "rep", n_rep, bit)
        for bit in bits_of(n_blk):
            prev = joined(prev, swap(prev, "blk", n_blk, bit), "blk", bit, 0)
        for axis, size in (("rep", n_rep), ("sub", n_sub)):
            for bit in bits_of(size):
                prev = joined(prev, swap(prev, axis, size, bit), axis, bit, 1)
        return (new_params, new_momentum, prev)

    return per_device


def solution(mesh):
    in_specs = (
        P(("groups", "blk", "rep", "sub"), None, None),
        P(("groups", "blk"), None),
        P(("groups", "blk"), None),
        P(("groups", "blk"), None),
    )
    out_specs = (P(("groups", "blk"), None), P(("groups", "blk"), None), P("groups", None))
    return jax.shard_map(
        make(mesh), mesh=mesh, in_specs=in_specs, out_specs=out_specs, check_vma=False
    )
```

```python
import functools

import jax
import jax.numpy as jnp
from jax import lax
from jax.experimental import pallas as pl
from jax.experimental.pallas import tpu as pltpu
from jax.sharding import PartitionSpec as P

momentum_coef = 0.9
outer_rate = 0.7
F32 = jnp.float32
BF16 = jnp.bfloat16
LANES = 128
GROUP = ("blk", "rep", "sub")


def bits_of(size):
    return [1 << k for k in range(size.bit_length() - 1)]


def mine(axis, bit):
    return (lax.axis_index(axis) & bit) // bit


def halves(value, axis, bit):
    half = value.shape[1] // 2
    at = mine(axis, bit) * half
    keep = lax.dynamic_slice_in_dim(value, at, half, 1)
    away = lax.dynamic_slice_in_dim(value, half - at, half, 1)
    return keep, away


def joined(own, other, axis, bit, dim):
    upper = mine(axis, bit) == 1
    return jnp.concatenate(
        [jnp.where(upper, other, own), jnp.where(upper, own, other)], axis=dim
    )


def squares_of(total, rows):
    sq = total * total
    sq = jnp.pad(sq, ((0, 0), (0, -sq.shape[1] % LANES)))
    sq = sum(sq[:, k : k + LANES] for k in range(0, sq.shape[1], LANES))
    return jnp.sum(sq.reshape(-1, rows, LANES), axis=0)


def finish(entries, at_ref, own_ref, rep_ref, sub_ref, both_ref, m_ref, p_ref, np_ref, nm_ref, np_buf, nm_buf, sems):
    width = own_ref.shape[1] - 2 * LANES

    def squares(ref):
        return ref[:, width : width + LANES].astype(F32) + ref[:, width + LANES :].astype(F32)

    total = (squares(own_ref) + squares(rep_ref)) + (squares(sub_ref) + squares(both_ref))
    total = jnp.sum(jnp.sum(total, axis=0, keepdims=True), axis=1, keepdims=True)
    clip_factor = jnp.minimum(
        1.0, jnp.sqrt(jnp.full((1, 1), entries, F32)) / jnp.sqrt(total + 1e-06)
    )
    at = at_ref[0]
    for k, ref in enumerate((own_ref, rep_ref, sub_ref, both_ref)):
        cols = pl.ds(pl.multiple_of((at ^ k) * width, LANES), width)
        scaled = clip_factor * ref[:, :width].astype(F32)
        new_momentum = momentum_coef * m_ref[:, cols] + scaled
        nm_buf[:, cols] = new_momentum
        np_buf[:, cols] = p_ref[:, cols] - outer_rate * (scaled + momentum_coef * new_momentum)
    copies = [
        pltpu.make_async_copy(nm_buf, nm_ref, sems.at[0]),
        pltpu.make_async_copy(np_buf, np_ref, sems.at[1]),
    ]
    for copy in copies:
        copy.start()
    for copy in copies:
        copy.wait()


def make(mesh):
    n_blk, n_rep, n_sub = (mesh.shape[a] for a in GROUP)

    def swap(value, blk=0, rep=0, sub=0):
        pairs = []
        for i in range(n_blk * n_rep * n_sub):
            b, r, s = i // (n_rep * n_sub), i // n_sub % n_rep, i % n_sub
            pairs.append((i, ((b ^ blk) * n_rep + (r ^ rep)) * n_sub + (s ^ sub)))
        return lax.ppermute(value, GROUP, pairs)

    def per_device(replica_delta, momentum, params, prev_master):
        return step(replica_delta, momentum, params, prev_master)

    def step(replica_delta, momentum, params, prev_master):
        delta = replica_delta[0]
        rows, width = momentum.shape
        entries = delta.shape[0] * width

        other = swap(delta, sub=1)
        half, _ = halves(delta, "sub", 1)
        half = lax.optimization_barrier(half)
        prev = prev_master.astype(BF16)
        prev, _ = halves(prev, "sub", 1)
        other, prev = lax.optimization_barrier((other, prev))
        total = half.astype(F32) + halves(other, "sub", 1)[0].astype(F32)

        total, away = halves(total, "rep", 1)
        sent, away = total.astype(BF16), away.astype(BF16)
        got = (swap(away, rep=1), swap(sent, blk=1), swap(away, rep=1, blk=1))
        total = total + got[0].astype(F32) + got[1].astype(F32) + got[2].astype(F32)
        for bit in bits_of(n_rep)[1:]:
            total, away = halves(total, "rep", bit)
            total = total + swap(away.astype(BF16), rep=bit).astype(F32)
        for bit in bits_of(n_blk)[1:]:
            total = total + swap(total.astype(BF16), blk=bit).astype(F32)

        squares = squares_of(total, rows)
        own = lax.dynamic_slice_in_dim(total, lax.axis_index("blk") * rows, rows, 0).astype(BF16)

        def pack(own, squares):
            high = lax.reduce_precision(squares, 8, 7)
            return jnp.concatenate([own, high.astype(BF16), (squares - high).astype(BF16)], axis=1)

        for bit in reversed(bits_of(n_rep)[1:]):
            packed = swap(pack(own, squares), rep=bit)
            n = own.shape[1]
            own = joined(own, packed[:, :n], "rep", bit, 1)
            squares = squares + packed[:, n : n + LANES].astype(F32) + packed[:, n + LANES :].astype(F32)
        packed = pack(own, squares)
        from_rep = swap(packed, rep=1)
        from_sub = swap(packed, sub=1)
        from_both = swap(packed, rep=1, sub=1)

        for bit in reversed(bits_of(n_blk)):
            prev = joined(prev, swap(prev, blk=bit), "blk", bit, 0)
        order = [sum(((b >> k) & 1) * (n_blk >> (k + 1)) for k in range(n_blk.bit_length() - 1)) for b in range(n_blk)]
        prev = jnp.concatenate([prev[o * rows : (o + 1) * rows] for o in order], axis=0)
        prev_other = swap(prev, sub=1)
        prev = joined(prev, prev_other, "sub", 1, 1)

        at = (2 * lax.axis_index("sub") + mine("rep", 1)).reshape(1)
        vmem, hbm = pl.BlockSpec(memory_space=pltpu.VMEM), pl.BlockSpec(memory_space=pl.ANY)
        out = jax.ShapeDtypeStruct(params.shape, F32)
        new_params, new_momentum = pl.pallas_call(
            functools.partial(finish, float(entries)),
            out_shape=(out, out),
            in_specs=[pl.BlockSpec(memory_space=pltpu.SMEM)] + [vmem] * 6,
            out_specs=(hbm, hbm),
            scratch_shapes=[
                pltpu.VMEM(params.shape, F32),
                pltpu.VMEM(params.shape, F32),
                pltpu.SemaphoreType.DMA((2,)),
            ],
            compiler_params=pltpu.CompilerParams(vmem_limit_bytes=4 << 20),
        )(at, packed, from_rep, from_sub, from_both, momentum, params)
        return (new_params, new_momentum, prev)

    return per_device


def solution(mesh):
    in_specs = (
        P(("groups", "blk", "rep", "sub"), None, None),
        P(("groups", "blk"), None),
        P(("groups", "blk"), None),
        P(("groups", "blk"), None),
    )
    out_specs = (P(("groups", "blk"), None), P(("groups", "blk"), None), P("groups", None))
    return jax.shard_map(
        make(mesh), mesh=mesh, in_specs=in_specs, out_specs=out_specs, check_vma=False
    )
```

```python
import functools

import jax
import jax.numpy as jnp
from jax import lax
from jax.experimental import pallas as pl
from jax.experimental.pallas import tpu as pltpu
from jax.sharding import PartitionSpec as P

momentum_coef = 0.9
outer_rate = 0.7
F32 = jnp.float32
BF16 = jnp.bfloat16
LANES = 128
GROUP = ("blk", "rep", "sub")


def bits_of(size):
    return [1 << k for k in range(size.bit_length() - 1)]


def mine(axis, bit):
    return (lax.axis_index(axis) & bit) // bit


def halves(value, axis, bit):
    half = value.shape[1] // 2
    at = mine(axis, bit) * half
    keep = lax.dynamic_slice_in_dim(value, at, half, 1)
    away = lax.dynamic_slice_in_dim(value, half - at, half, 1)
    return keep, away


def joined(own, other, axis, bit, dim):
    upper = mine(axis, bit) == 1
    return jnp.concatenate(
        [jnp.where(upper, other, own), jnp.where(upper, own, other)], axis=dim
    )


def squares_of(total, rows):
    sq = total * total
    sq = jnp.pad(sq, ((0, 0), (0, -sq.shape[1] % LANES)))
    sq = sum(sq[:, k : k + LANES] for k in range(0, sq.shape[1], LANES))
    return jnp.sum(sq.reshape(-1, rows, LANES), axis=0)


def finish(entries, at_ref, own_ref, rep_ref, sub_ref, both_ref, base_m_ref, base_p_ref, np_ref, nm_ref, np_buf, nm_buf, sems):
    width = own_ref.shape[1] - 2 * LANES

    def squares(ref):
        return ref[:, width : width + LANES].astype(F32) + ref[:, width + LANES :].astype(F32)

    total = (squares(own_ref) + squares(rep_ref)) + (squares(sub_ref) + squares(both_ref))
    total = jnp.sum(jnp.sum(total, axis=0, keepdims=True), axis=1, keepdims=True)
    clip_factor = jnp.minimum(
        1.0, jnp.sqrt(jnp.full((1, 1), entries, F32)) / jnp.sqrt(total + 1e-06)
    )
    at = at_ref[0]
    copies = []
    for k, ref in enumerate((own_ref, rep_ref, sub_ref, both_ref)):
        cols = pl.ds(pl.multiple_of((at ^ k) * width, LANES), width)
        scaled = clip_factor * ref[:, :width].astype(F32)
        nm_buf[:, cols] = base_m_ref[:, cols] + scaled
        np_buf[:, cols] = base_p_ref[:, cols] - outer_rate * (1.0 + momentum_coef) * scaled
        for j, (buf, ref) in enumerate(((nm_buf, nm_ref), (np_buf, np_ref))):
            copies.append(pltpu.make_async_copy(buf.at[:, cols], ref.at[:, cols], sems.at[2 * k + j]))
            copies[-1].start()
    for copy in copies:
        copy.wait()


def make(mesh):
    n_blk, n_rep, n_sub = (mesh.shape[a] for a in GROUP)

    def swap(value, blk=0, rep=0, sub=0):
        pairs = []
        for i in range(n_blk * n_rep * n_sub):
            b, r, s = i // (n_rep * n_sub), i // n_sub % n_rep, i % n_sub
            pairs.append((i, ((b ^ blk) * n_rep + (r ^ rep)) * n_sub + (s ^ sub)))
        return lax.ppermute(value, GROUP, pairs)

    def per_device(replica_delta, momentum, params, prev_master):
        return step(replica_delta, momentum, params, prev_master)

    def step(replica_delta, momentum, params, prev_master):
        delta = replica_delta[0]
        rows, width = momentum.shape
        entries = delta.shape[0] * width

        other = swap(delta, sub=1)
        half, _ = halves(delta, "sub", 1)
        half = lax.optimization_barrier(half)
        prev = prev_master.astype(BF16)
        prev, _ = halves(prev, "sub", 1)
        other, prev = lax.optimization_barrier((other, prev))
        total = half.astype(F32) + halves(other, "sub", 1)[0].astype(F32)

        total, away = halves(total, "rep", 1)
        sent, away = total.astype(BF16), away.astype(BF16)
        got = (swap(away, rep=1), swap(sent, blk=1), swap(away, rep=1, blk=1))
        total = total + got[0].astype(F32) + got[1].astype(F32) + got[2].astype(F32)
        for bit in bits_of(n_rep)[1:]:
            total, away = halves(total, "rep", bit)
            total = total + swap(away.astype(BF16), rep=bit).astype(F32)
        for bit in bits_of(n_blk)[1:]:
            sent = total.astype(BF16)
            got_far = swap(sent, blk=bit)
            total = total + got_far.astype(F32)

        squares = squares_of(total, rows)
        own = lax.dynamic_slice_in_dim(total, lax.axis_index("blk") * rows, rows, 0).astype(BF16)

        def pack(own, squares):
            high = lax.reduce_precision(squares, 8, 7)
            return jnp.concatenate([own, high.astype(BF16), (squares - high).astype(BF16)], axis=1)

        for bit in reversed(bits_of(n_rep)[1:]):
            packed = swap(pack(own, squares), rep=bit)
            n = own.shape[1]
            own = joined(own, packed[:, :n], "rep", bit, 1)
            squares = squares + packed[:, n : n + LANES].astype(F32) + packed[:, n + LANES :].astype(F32)
        packed = pack(own, squares)
        from_rep = swap(packed, rep=1)
        from_sub = swap(packed, sub=1)
        from_both = swap(packed, rep=1, sub=1)

        for bit in reversed(bits_of(n_blk)):
            prev = joined(prev, swap(prev, blk=bit), "blk", bit, 0)
        order = [sum(((b >> k) & 1) * (n_blk >> (k + 1)) for k in range(n_blk.bit_length() - 1)) for b in range(n_blk)]
        prev = jnp.concatenate([prev[o * rows : (o + 1) * rows] for o in order], axis=0)
        prev_other = swap(prev, sub=1)
        prev = joined(prev, prev_other, "sub", 1, 1)

        base_m = momentum_coef * momentum
        base_p = params - outer_rate * momentum_coef * base_m
        at = (2 * lax.axis_index("sub") + mine("rep", 1)).reshape(1)
        vmem, hbm = pl.BlockSpec(memory_space=pltpu.VMEM), pl.BlockSpec(memory_space=pl.ANY)
        out = jax.ShapeDtypeStruct(params.shape, F32)
        new_params, new_momentum = pl.pallas_call(
            functools.partial(finish, float(entries)),
            out_shape=(out, out),
            in_specs=[pl.BlockSpec(memory_space=pltpu.SMEM)] + [vmem] * 6,
            out_specs=(hbm, hbm),
            scratch_shapes=[
                pltpu.VMEM(params.shape, F32),
                pltpu.VMEM(params.shape, F32),
                pltpu.SemaphoreType.DMA((8,)),
            ],
            compiler_params=pltpu.CompilerParams(vmem_limit_bytes=4 << 20),
        )(at, packed, from_rep, from_sub, from_both, base_m, base_p)
        return (new_params, new_momentum, prev)

    return per_device


def solution(mesh):
    in_specs = (
        P(("groups", "blk", "rep", "sub"), None, None),
        P(("groups", "blk"), None),
        P(("groups", "blk"), None),
        P(("groups", "blk"), None),
    )
    out_specs = (P(("groups", "blk"), None), P(("groups", "blk"), None), P("groups", None))
    return jax.shard_map(
        make(mesh), mesh=mesh, in_specs=in_specs, out_specs=out_specs, check_vma=False
    )
```

```python
import functools

import jax
import jax.numpy as jnp
from jax import lax
from jax.experimental import pallas as pl
from jax.experimental.pallas import tpu as pltpu
from jax.sharding import PartitionSpec as P

momentum_coef = 0.9
outer_rate = 0.7
F32 = jnp.float32
BF16 = jnp.bfloat16
LANES = 128
GROUP = ("blk", "rep", "sub")


def bits_of(size):
    return [1 << k for k in range(size.bit_length() - 1)]


def mine(axis, bit):
    return (lax.axis_index(axis) & bit) // bit


def halves(value, axis, bit):
    half = value.shape[1] // 2
    at = mine(axis, bit) * half
    keep = lax.dynamic_slice_in_dim(value, at, half, 1)
    away = lax.dynamic_slice_in_dim(value, half - at, half, 1)
    return keep, away


def joined(own, other, axis, bit, dim):
    upper = mine(axis, bit) == 1
    return jnp.concatenate(
        [jnp.where(upper, other, own), jnp.where(upper, own, other)], axis=dim
    )


def squares_of(total, rows):
    sq = total * total
    sq = jnp.pad(sq, ((0, 0), (0, -sq.shape[1] % LANES)))
    sq = sum(sq[:, k : k + LANES] for k in range(0, sq.shape[1], LANES))
    return jnp.sum(sq.reshape(-1, rows // 2, LANES), axis=0)


def finish(entries, at_ref, own_ref, rep_ref, sub_ref, both_ref, base_m_ref, base_p_ref, prev_ref, prev_other_ref,
           np_ref, nm_ref, prev_out_ref, np_buf, nm_buf, sems):
    width = own_ref.shape[1] - LANES
    half = prev_ref.shape[1]
    at = at_ref[0]
    copies = []
    for k, ref in enumerate((prev_ref, prev_other_ref)):
        cols = pl.ds(pl.multiple_of(((at // 2) ^ k) * half, LANES), half)
        copies.append(pltpu.make_async_copy(ref, prev_out_ref.at[:, cols], sems.at[8 + k]))
        copies[-1].start()

    def squares(ref):
        both = ref[:, width:].astype(F32)
        return both[: both.shape[0] // 2] + both[both.shape[0] // 2 :]

    total = (squares(own_ref) + squares(rep_ref)) + (squares(sub_ref) + squares(both_ref))
    total = jnp.sum(jnp.sum(total, axis=0, keepdims=True), axis=1, keepdims=True)
    clip_factor = jnp.minimum(
        1.0, jnp.sqrt(jnp.full((1, 1), entries, F32)) / jnp.sqrt(total + 1e-06)
    )
    for k, ref in enumerate((own_ref, rep_ref, sub_ref, both_ref)):
        cols = pl.ds(pl.multiple_of((at ^ k) * width, LANES), width)
        scaled = clip_factor * ref[:, :width].astype(F32)
        nm_buf[:, cols] = base_m_ref[:, cols] + scaled
        np_buf[:, cols] = base_p_ref[:, cols] - outer_rate * (1.0 + momentum_coef) * scaled
        for j, (buf, ref) in enumerate(((nm_buf, nm_ref), (np_buf, np_ref))):
            copies.append(pltpu.make_async_copy(buf.at[:, cols], ref.at[:, cols], sems.at[2 * k + j]))
            copies[-1].start()
    for copy in copies:
        copy.wait()


def make(mesh):
    n_blk, n_rep, n_sub = (mesh.shape[a] for a in GROUP)

    def swap(value, blk=0, rep=0, sub=0):
        pairs = []
        for i in range(n_blk * n_rep * n_sub):
            b, r, s = i // (n_rep * n_sub), i // n_sub % n_rep, i % n_sub
            pairs.append((i, ((b ^ blk) * n_rep + (r ^ rep)) * n_sub + (s ^ sub)))
        return lax.ppermute(value, GROUP, pairs)

    def per_device(replica_delta, momentum, params, prev_master):
        return step(replica_delta, momentum, params, prev_master)

    def step(replica_delta, momentum, params, prev_master):
        delta = replica_delta[0]
        rows, width = momentum.shape
        entries = delta.shape[0] * width

        other = swap(delta, sub=1)
        half, _ = halves(delta, "sub", 1)
        half = lax.optimization_barrier(half)
        prev = prev_master.astype(BF16)
        prev, _ = halves(prev, "sub", 1)
        other, prev = lax.optimization_barrier((other, prev))
        total = half.astype(F32) + halves(other, "sub", 1)[0].astype(F32)

        total, away = halves(total, "rep", 1)
        sent, away = total.astype(BF16), away.astype(BF16)
        got = (swap(away, rep=1), swap(sent, blk=1), swap(away, rep=1, blk=1))
        total = total + got[0].astype(F32) + got[1].astype(F32) + got[2].astype(F32)
        for bit in bits_of(n_rep)[1:]:
            total, away = halves(total, "rep", bit)
            total = total + swap(away.astype(BF16), rep=bit).astype(F32)
        for bit in bits_of(n_blk)[1:]:
            sent = total.astype(BF16)
            got_far = swap(sent, blk=bit)
            total = total + got_far.astype(F32)

        squares = squares_of(total, rows)
        own = lax.dynamic_slice_in_dim(total, lax.axis_index("blk") * rows, rows, 0).astype(BF16)

        def pack(own, squares):
            high = lax.reduce_precision(squares, 8, 7)
            both = jnp.concatenate([high, squares - high], axis=0).astype(BF16)
            return jnp.concatenate([own, both], axis=1)

        for bit in reversed(bits_of(n_rep)[1:]):
            packed = swap(pack(own, squares), rep=bit)
            n = own.shape[1]
            own = joined(own, packed[:, :n], "rep", bit, 1)
            both = packed[:, n:].astype(F32)
            squares = squares + both[: rows // 2] + both[rows // 2 :]
        packed = pack(own, squares)
        from_rep = swap(packed, rep=1)
        from_sub = swap(packed, sub=1)
        from_both = swap(packed, rep=1, sub=1)

        for bit in reversed(bits_of(n_blk)):
            prev = joined(prev, swap(prev, blk=bit), "blk", bit, 0)
        order = [sum(((b >> k) & 1) * (n_blk >> (k + 1)) for k in range(n_blk.bit_length() - 1)) for b in range(n_blk)]
        prev = jnp.concatenate([prev[o * rows : (o + 1) * rows] for o in order], axis=0)
        prev_other = swap(prev, sub=1)

        base_m = momentum_coef * momentum
        base_p = params - outer_rate * momentum_coef * base_m
        at = (2 * lax.axis_index("sub") + mine("rep", 1)).reshape(1)
        vmem, hbm = pl.BlockSpec(memory_space=pltpu.VMEM), pl.BlockSpec(memory_space=pl.ANY)
        out = jax.ShapeDtypeStruct(params.shape, F32)
        new_params, new_momentum, prev = pl.pallas_call(
            functools.partial(finish, float(entries)),
            out_shape=(out, out, jax.ShapeDtypeStruct((prev.shape[0], width), BF16)),
            in_specs=[pl.BlockSpec(memory_space=pltpu.SMEM)] + [vmem] * 8,
            out_specs=(hbm, hbm, hbm),
            scratch_shapes=[
                pltpu.VMEM(params.shape, F32),
                pltpu.VMEM(params.shape, F32),
                pltpu.SemaphoreType.DMA((10,)),
            ],
            compiler_params=pltpu.CompilerParams(vmem_limit_bytes=4 << 20),
        )(at, packed, from_rep, from_sub, from_both, base_m, base_p, prev, prev_other)
        return (new_params, new_momentum, prev)

    return per_device


def solution(mesh):
    in_specs = (
        P(("groups", "blk", "rep", "sub"), None, None),
        P(("groups", "blk"), None),
        P(("groups", "blk"), None),
        P(("groups", "blk"), None),
    )
    out_specs = (P(("groups", "blk"), None), P(("groups", "blk"), None), P("groups", None))
    return jax.shard_map(
        make(mesh), mesh=mesh, in_specs=in_specs, out_specs=out_specs, check_vma=False
    )
```
